32 devices in a mesh: height: 4 (over x, core), dom: 8 (over z, y).
Axes of the slice: x: 2, y: 2, z: 4, core: 2. Of those that a mesh axis runs over, the one named last changes fastest.
Arguments:
- modes_now: float32 [64, 64, 4096], P('height', 'dom'), may hold values from -6 to 6
- modes_prev: float32 [64, 64, 4096], P('height', 'dom'), may hold values from -6 to 6
- partition_boxes: int32 [64, 2], P('dom'), may hold values from 16 to 64, as said below
- face_table: int32 [256, 8], P('dom'), may hold values from 0 to 64, as said below
Outputs:
- new_modes: float32 [64, 64, 4096], P('height', 'dom')
- pressure: float32 [64, 64, 4096], P('height', 'dom')
The draws below stay inside these ranges and needn't reach their ends.
Inputs may be any that keep to these rules, and one draw needn't show every extreme that they name: `partition_boxes`: column 0 is a partition's extent along x, column 1 along y. `face_table`: row r belongs to dom index r // 32. Columns: 0 the local number of the source partition on that index, 1 its side (0 low x, 1 high x, 2 low y, 3 high y), 2 the first cell of the face along that side, 3 the face's length in cells (0 marks an unused row), 4 the dom index holding the target partition, 5 the target's local number, 6 its side, 7 the first cell along it. Sides 0 and 1 run along y, sides 2 and 3 along x; start plus length never passes either side's extent. Among the rows of one dom index at most 4 name the same dom index in column 4, and that many is reached in every draw.
All inputs are finite; a program needn't handle non-finite values.
Results may differ from the reference program's by a relative error of at most 0.0002.
Values sent between devices are 32-bit elements; how exact they have to be, the bound alone decides.
A program may use at most 64 MiB of HBM per device.

```python
import jax
import jax.numpy as jnp
from jax import lax

B = 64
NZ = 64
PDEV = 8
FDEV = 32
PARTS_SIZE = 64
N_DOM = 8


def layout_tables(key):
    extents = jax.random.randint(jax.random.fold_in(key, 101), (N_DOM * PDEV, 2), B // 4, B + 1)
    pair_most = max(2, FDEV // N_DOM)
    groups = FDEV // pair_most
    order_key = jax.random.fold_in(key, 202)
    sources = jnp.arange(N_DOM, dtype=jnp.int32)

    def shuffled(source):
        return jax.random.permutation(jax.random.fold_in(order_key, source), N_DOM).astype(jnp.int32)
    offsets = jax.vmap(shuffled)(sources)[:, :groups]
    slot_ids = jnp.arange(FDEV, dtype=jnp.int32)
    group_of = slot_ids // pair_most
    targets = (sources[:, None] + offsets[:, group_of]) % N_DOM
    live_count = jax.random.randint(jax.random.fold_in(key, 303), (N_DOM, groups), 1, pair_most + 1)
    live_count = live_count.at[:, 0].set(pair_most)
    alive = (slot_ids % pair_most)[None, :] < live_count[:, group_of]
    grid_shape = (N_DOM, FDEV)
    src_part = jax.random.randint(jax.random.fold_in(key, 404), grid_shape, 0, PDEV)
    src_side = jax.random.randint(jax.random.fold_in(key, 505), grid_shape, 0, 4)
    dst_part = jax.random.randint(jax.random.fold_in(key, 606), grid_shape, 0, PDEV)
    dst_side = jax.random.randint(jax.random.fold_in(key, 707), grid_shape, 0, 4)
    src_global = sources[:, None] * PDEV + src_part
    dst_global = targets * PDEV + dst_part
    src_extent = jnp.where(src_side < 2, extents[src_global, 1], extents[src_global, 0])
    dst_extent = jnp.where(dst_side < 2, extents[dst_global, 1], extents[dst_global, 0])
    seg_length = jax.random.randint(jax.random.fold_in(key, 808), grid_shape, 1, jnp.minimum(src_extent, dst_extent) + 1)
    seg_length = jnp.where(alive, seg_length, 0)
    src_start = jax.random.randint(jax.random.fold_in(key, 909), grid_shape, 0, src_extent - seg_length + 1)
    dst_start = jax.random.randint(jax.random.fold_in(key, 1001), grid_shape, 0, dst_extent - seg_length + 1)
    face_rows = jnp.stack([src_part, src_side, src_start, seg_length, targets, dst_part, dst_side, dst_start], -1)
    return (extents.astype(jnp.int32), face_rows.reshape(N_DOM * FDEV, 8).astype(jnp.int32))


def draw_partition_boxes(key, part):
    return layout_tables(key)[0]


def draw_face_table(key, part):
    return layout_tables(key)[1]


def block_levels(stream_key, extent, pieces, smallest, largest):
    def one(dim, parts):
        steps = jax.random.uniform(jax.random.fold_in(jax.random.fold_in(stream_key, 6), dim), (parts,), jnp.float32, smallest / len(pieces), largest / len(pieces))
        return jnp.repeat(jnp.exp(steps), extent[dim] // parts).reshape((-1,) + (1,) * (len(extent) - dim - 1))

    gain = one(*pieces[0])
    for cut in pieces[1:]:
        gain = gain * one(*cut)
    return gain


def centred(own_key, dims, spread, most, pieces=(), held_as=jnp.bfloat16):
    entries = jax.random.normal(own_key, dims, jnp.float32) * spread
    if len(pieces) > 0:
        entries = block_levels(own_key, dims, pieces, -0.22, 0.18) * entries
    return jnp.clip(entries, min=-most, max=most).astype(held_as)


def setup_inputs(seed: int = 0) -> dict:
    arg_keys = jax.random.split(jax.random.key(seed), 5)
    return {
        "modes_now": centred(arg_keys[0], (NZ, PARTS_SIZE, B * B), 1.0, 6.0, ((0, 4), (1, 8)), jnp.float32),
        "modes_prev": centred(arg_keys[1], (NZ, PARTS_SIZE, B * B), 1.0, 6.0, ((0, 4), (1, 8)), jnp.float32),
        "partition_boxes": draw_partition_boxes(jax.random.fold_in(arg_keys[4], 71), 0),
        "face_table": draw_face_table(jax.random.fold_in(arg_keys[4], 71), 0),
    }


COUPLING = 32.0
STENCIL = (COUPLING * 270.0 / 180.0, COUPLING * -27.0 / 180.0, COUPLING * 2.0 / 180.0)
TIME_STEP = 0.4

def cosine_table(lengths, box_side):
    lengths = lengths.astype(jnp.float32)[..., None, None]
    ordinal = jnp.arange(box_side, dtype=jnp.float32)
    waves = ordinal[:, None]
    places = ordinal[None, :]
    scales = jnp.sqrt(jnp.where(waves == 0, 1.0, 2.0) / lengths)
    values = scales * jnp.cos(jnp.pi * waves * (places + 0.5) / lengths)
    inside = (waves < lengths) & (places < lengths)
    return jnp.where(inside, values, 0.0)

def mix_planes(matrix, grid_field):
    flat = grid_field.reshape(matrix.shape[1], -1)
    mixed = jnp.dot(matrix, flat, precision=lax.Precision.HIGHEST, preferred_element_type=jnp.float32)
    return mixed.reshape(matrix.shape[0], grid_field.shape[1], grid_field.shape[2])

def to_cells(table_rows, table_cols, grid_field, box_side):
    planes, holders, cells = grid_field.shape
    squares = grid_field.reshape(planes, holders, box_side, box_side)
    halfway = jnp.einsum('pka,zpkl->zpal', table_rows, squares, precision=lax.Precision.HIGHEST)
    complete = jnp.einsum('zpal,plb->zpab', halfway, table_cols, precision=lax.Precision.HIGHEST)
    return complete.reshape(planes, holders, cells)

def to_modes(table_rows, table_cols, grid_field, box_side):
    planes, holders, cells = grid_field.shape
    squares = grid_field.reshape(planes, holders, box_side, box_side)
    halfway = jnp.einsum('pka,zpab->zpkb', table_rows, squares, precision=lax.Precision.HIGHEST)
    complete = jnp.einsum('zpkb,plb->zpkl', halfway, table_cols, precision=lax.Precision.HIGHEST)
    return complete.reshape(planes, holders, cells)

def side_cells(facing, offsets, amounts, extent_rows, extent_cols, box_side):
    number = facing.shape[0]
    layers = jnp.arange(3, dtype=jnp.int32)[None, :, None]
    position = jnp.arange(box_side, dtype=jnp.int32)[None, None, :]
    facing = facing[:, None, None]
    reached = offsets[:, None, None] + position
    coord_rows = jnp.where(facing == 0, layers, jnp.where(facing == 1, extent_rows[:, None, None] - 1 - layers, reached))
    coord_cols = jnp.where(facing == 2, layers, jnp.where(facing == 3, extent_cols[:, None, None] - 1 - layers, reached))
    usable = jnp.broadcast_to((position < amounts[:, None, None]) & (layers >= 0), (number, 3, box_side))
    cell_index = jnp.where(usable, coord_rows * box_side + coord_cols, 0)
    return (cell_index.reshape(number, 3 * box_side).astype(jnp.int32), usable.reshape(number, 3 * box_side))

def face_forcing(pressure, aligned, targets, facing, offsets, amounts, extent_rows, extent_cols, box_side):
    planes = pressure.shape[0]
    number = targets.shape[0]
    cell_index, usable = side_cells(facing, offsets, amounts, extent_rows[targets], extent_cols[targets], box_side)
    inside_rim = jnp.where(usable, pressure[:, targets[:, None], cell_index], 0.0)
    jumps = (aligned - inside_rim).reshape(planes, number, 3, box_side)
    nearest = jumps[:, :, 0]
    second = jumps[:, :, 1]
    farthest = jumps[:, :, 2]
    closest = STENCIL[0] * nearest + STENCIL[1] * second + STENCIL[2] * farthest
    middle = STENCIL[1] * nearest + STENCIL[2] * second
    outer = STENCIL[2] * nearest
    pushes = jnp.stack([closest, middle, outer], 2).reshape(planes, number, 3 * box_side)
    pushes = jnp.where(usable, pushes, 0.0)
    return jnp.zeros_like(pressure).at[:, targets[:, None], cell_index].add(pushes)

def advance(modes_now, modes_prev, force_modes, extent_rows, extent_cols, first_plane, total_planes, box_side):
    planes, holders, cells = modes_now.shape
    wave_depth = (first_plane + jnp.arange(planes, dtype=jnp.int32)).astype(jnp.float32) / total_planes
    wave_side = jnp.arange(box_side, dtype=jnp.float32)
    float_rows = extent_rows.astype(jnp.float32)
    float_cols = extent_cols.astype(jnp.float32)
    ratio_rows = wave_side[None, :] / float_rows[:, None]
    ratio_cols = wave_side[None, :] / float_cols[:, None]
    squared = jnp.pi ** 2 * (wave_depth[:, None, None, None] ** 2 + ratio_rows[None, :, :, None] ** 2 + ratio_cols[None, :, None, :] ** 2)
    phases = jnp.sqrt(squared) * TIME_STEP
    growth = TIME_STEP * TIME_STEP * jnp.sinc(phases / (2.0 * jnp.pi)) ** 2
    inside = (wave_side[None, :, None] < float_rows[:, None, None]) & (wave_side[None, None, :] < float_cols[:, None, None])
    grid_shape = (planes, holders, box_side, box_side)
    updated = 2.0 * jnp.cos(phases) * modes_now.reshape(grid_shape) - modes_prev.reshape(grid_shape) + growth * force_modes.reshape(grid_shape)
    return jnp.where(inside[None], updated, 0.0).reshape(planes, holders, cells)

def reference(modes_now, modes_prev, partition_boxes, face_table):
    extent_rows = partition_boxes[:, 0]
    extent_cols = partition_boxes[:, 1]
    table_rows = cosine_table(extent_rows, B)
    table_cols = cosine_table(extent_cols, B)
    table_depth = cosine_table(jnp.full((), NZ, jnp.int32), NZ)
    plane_modes = mix_planes(table_depth.T, modes_now)
    pressure = to_cells(table_rows, table_cols, plane_modes, B)
    row_ids = jnp.arange(N_DOM * FDEV, dtype=jnp.int32)
    holder = row_ids // FDEV
    sources = holder * PDEV + face_table[:, 0]
    src_index, src_usable = side_cells(face_table[:, 1], face_table[:, 2], face_table[:, 3], extent_rows[sources], extent_cols[sources], B)
    aligned = jnp.where(src_usable, pressure[:, sources[:, None], src_index], 0.0)
    targets = face_table[:, 4] * PDEV + face_table[:, 5]
    forcing = face_forcing(pressure, aligned, targets, face_table[:, 6], face_table[:, 7], face_table[:, 3], extent_rows, extent_cols, B)
    force_modes = mix_planes(table_depth, to_modes(table_rows, table_cols, forcing, B))
    new_modes = advance(modes_now, modes_prev, force_modes, extent_rows, extent_cols, jnp.zeros((), jnp.int32), NZ, B)
    return (new_modes, pressure)
```

```python
import jax
import jax.numpy as jnp
from jax import lax
from jax.sharding import PartitionSpec as P

B = 64


COUPLING = 32.0
STENCIL = (COUPLING * 270.0 / 180.0, COUPLING * -27.0 / 180.0, COUPLING * 2.0 / 180.0)
TIME_STEP = 0.4


def cosine_table(lengths, box_side):
    lengths = lengths.astype(jnp.float32)[..., None, None]
    ordinal = jnp.arange(box_side, dtype=jnp.float32)
    waves = ordinal[:, None]
    places = ordinal[None, :]
    scales = jnp.sqrt(jnp.where(waves == 0, 1.0, 2.0) / lengths)
    values = scales * jnp.cos(jnp.pi * waves * (places + 0.5) / lengths)
    inside = (waves < lengths) & (places < lengths)
    return jnp.where(inside, values, 0.0)


def to_cells(table_rows, table_cols, grid_field, box_side):
    planes, holders, cells = grid_field.shape
    squares = grid_field.reshape(planes, holders, box_side, box_side)
    halfway = jnp.einsum("pka,zpkl->zpal", table_rows, squares, precision=lax.Precision.HIGH)
    complete = jnp.einsum("zpal,plb->zpab", halfway, table_cols, precision=lax.Precision.HIGH)
    return complete.reshape(planes, holders, cells)


def to_modes(table_rows, table_cols, grid_field, box_side):
    planes, holders, cells = grid_field.shape
    squares = grid_field.reshape(planes, holders, box_side, box_side)
    halfway = jnp.einsum("pka,zpab->zpkb", table_rows, squares, precision=lax.Precision.HIGH)
    complete = jnp.einsum("zpkb,plb->zpkl", halfway, table_cols, precision=lax.Precision.HIGH)
    return complete.reshape(planes, holders, cells)


def depth_mix(grid_field, matrix):
    total_planes = matrix.shape[0]
    pieces = lax.all_to_all(grid_field, "height", split_axis=1, concat_axis=0, tiled=True)
    combined = jnp.dot(
        matrix,
        pieces.reshape(total_planes, -1),
        precision=lax.Precision.HIGH,
        preferred_element_type=jnp.float32,
    )
    return lax.all_to_all(
        combined.reshape(pieces.shape), "height", split_axis=0, concat_axis=1, tiled=True
    )


def side_selectors(extent_rows, extent_cols, box_side):
    holders = extent_rows.shape[0]
    layers = jnp.arange(3, dtype=jnp.int32)[None, :, None]
    place = jnp.arange(box_side, dtype=jnp.int32)[None, None, :]
    lowest = jnp.broadcast_to(place == layers, (holders, 3, box_side))
    high_rows = place == extent_rows[:, None, None] - 1 - layers
    high_cols = place == extent_cols[:, None, None] - 1 - layers
    select_rows = jnp.stack([lowest, high_rows], 1).astype(jnp.float32)
    select_cols = jnp.stack([lowest, high_cols], 1).astype(jnp.float32)
    return (select_rows, select_cols)


def side_stack(pressure, select_rows, select_cols, box_side):
    planes, holders, cells = pressure.shape
    squares = pressure.reshape(planes, holders, box_side, box_side)
    along_cols = jnp.einsum(
        "psjx,zpxy->zpsjy", select_rows, squares, precision=lax.Precision.HIGH
    )
    along_rows = jnp.einsum(
        "psjy,zpxy->zpsjx", select_cols, squares, precision=lax.Precision.HIGH
    )
    joined = jnp.concatenate([along_cols, along_rows], 2)
    return joined.reshape(planes, holders * 4, 3 * box_side)


def shifter(offsets, amounts, box_side):
    spot = jnp.arange(box_side, dtype=jnp.int32)[None, :, None]
    cellpos = jnp.arange(box_side, dtype=jnp.int32)[None, None, :]
    hits = (cellpos == offsets[:, None, None] + spot) & (spot < amounts[:, None, None])
    return hits.astype(jnp.float32)


def pick_rows(row_ids, count):
    return (row_ids[:, None] == jnp.arange(count, dtype=jnp.int32)[None, :]).astype(jnp.float32)


def select_faces(stacked, row_ids, offsets, amounts, box_side):
    planes, count, width = stacked.shape
    picked = jnp.einsum(
        "rk,zkm->zrm", pick_rows(row_ids, count), stacked, precision=lax.Precision.HIGH
    )
    picked = picked.reshape(planes, row_ids.shape[0], 3, box_side)
    return jnp.einsum(
        "rqc,zrjc->zrjq",
        shifter(offsets, amounts, box_side),
        picked,
        precision=lax.Precision.HIGH,
    )


def face_forcing(
    local_sides, aligned, targets, facing, offsets, amounts, select_rows, select_cols, box_side
):
    planes, count, width = local_sides.shape
    holders = count // 4
    number = targets.shape[0]
    target_ids = targets * 4 + facing
    inside_rim = select_faces(local_sides, target_ids, offsets, amounts, box_side)
    jumps = aligned - inside_rim
    nearest = jumps[:, :, 0]
    second = jumps[:, :, 1]
    farthest = jumps[:, :, 2]
    closest = STENCIL[0] * nearest + STENCIL[1] * second + STENCIL[2] * farthest
    middle = STENCIL[1] * nearest + STENCIL[2] * second
    outer = STENCIL[2] * nearest
    pushes = jnp.stack([closest, middle, outer], 2)
    placed = jnp.einsum(
        "rqc,zrjq->zrjc",
        shifter(offsets, amounts, box_side),
        pushes,
        precision=lax.Precision.HIGH,
    )
    placed = placed.reshape(planes, number, 3 * box_side)
    side_force = jnp.einsum(
        "rk,zrm->zkm", pick_rows(target_ids, count), placed, precision=lax.Precision.HIGH
    )
    side_force = side_force.reshape(planes, holders, 4, 3, box_side)
    from_cols = jnp.einsum(
        "psjx,zpsjy->zpxy", select_rows, side_force[:, :, 0:2], precision=lax.Precision.HIGH
    )
    from_rows = jnp.einsum(
        "psjy,zpsjx->zpxy", select_cols, side_force[:, :, 2:4], precision=lax.Precision.HIGH
    )
    return (from_cols + from_rows).reshape(planes, holders, box_side * box_side)


def interfaces(pressure, face_table, extent_rows, extent_cols):
    planes, holders, cells = pressure.shape
    listed = face_table.shape[0]
    dom_count = lax.axis_size("dom")
    pair_most = max(2, listed // dom_count)
    select_rows, select_cols = side_selectors(extent_rows, extent_cols, B)
    local_sides = side_stack(pressure, select_rows, select_cols, B)
    source_ids = face_table[:, 0] * 4 + face_table[:, 1]
    rim_values = select_faces(
        local_sides, source_ids, face_table[:, 2], face_table[:, 3], B
    ).reshape(planes, listed, 3 * B)
    targets = face_table[:, 4]
    matches = (targets[:, None] == jnp.arange(dom_count, dtype=jnp.int32)[None, :]).astype(
        jnp.int32
    )
    position_in = jnp.sum(jnp.cumsum(matches, 0) * matches, 1) - 1
    slot_ids = targets * pair_most + position_in
    slot_hits = (
        jnp.arange(dom_count * pair_most, dtype=jnp.int32)[:, None] == slot_ids[None, :]
    ).astype(jnp.int32)
    outgoing = jnp.einsum(
        "sr,zrm->zsm", slot_hits.astype(jnp.float32), rim_values, precision=lax.Precision.HIGH
    )
    labels = jnp.stack([face_table[:, 5], face_table[:, 6], face_table[:, 7], face_table[:, 3]], 1)
    label_slots = jnp.sum(slot_hits[:, :, None] * labels[None, :, :], 1)[None]
    label_plane = jnp.pad(label_slots.astype(jnp.float32), ((0, 0), (0, 0), (0, 3 * B - 4)))
    received = lax.all_to_all(
        jnp.concatenate([outgoing, label_plane], 0), "dom", split_axis=1, concat_axis=1, tiled=True
    )
    arrived = received[planes, :, :4].astype(jnp.int32)
    aligned = received[:planes].reshape(planes, dom_count * pair_most, 3, B)
    targets_here = arrived[:, 0]
    facing = arrived[:, 1]
    offsets = arrived[:, 2]
    lengths = arrived[:, 3]
    return face_forcing(
        local_sides, aligned, targets_here, facing, offsets, lengths, select_rows, select_cols, B
    )


def advance(
    modes_now,
    modes_prev,
    force_modes,
    extent_rows,
    extent_cols,
    first_plane,
    total_planes,
    box_side,
):
    planes, holders, cells = modes_now.shape
    wave_depth = (first_plane + jnp.arange(planes, dtype=jnp.int32)).astype(
        jnp.float32
    ) / total_planes
    wave_side = jnp.arange(box_side, dtype=jnp.float32)
    float_rows = extent_rows.astype(jnp.float32)
    float_cols = extent_cols.astype(jnp.float32)
    ratio_rows = wave_side[None, :] / float_rows[:, None]
    ratio_cols = wave_side[None, :] / float_cols[:, None]
    squared = jnp.pi**2 * (
        wave_depth[:, None, None, None] ** 2
        + ratio_rows[None, :, :, None] ** 2
        + ratio_cols[None, :, None, :] ** 2
    )
    phases = jnp.sqrt(squared) * TIME_STEP
    growth = TIME_STEP * TIME_STEP * jnp.sinc(phases / (2.0 * jnp.pi)) ** 2
    inside = (wave_side[None, :, None] < float_rows[:, None, None]) & (
        wave_side[None, None, :] < float_cols[:, None, None]
    )
    grid_shape = (planes, holders, box_side, box_side)
    updated = (
        2.0 * jnp.cos(phases) * modes_now.reshape(grid_shape)
        - modes_prev.reshape(grid_shape)
        + growth * force_modes.reshape(grid_shape)
    )
    return jnp.where(inside[None], updated, 0.0).reshape(planes, holders, cells)


def on_device(modes_now, modes_prev, partition_boxes, face_table):
    planes = modes_now.shape[0]
    total_planes = planes * lax.axis_size("height")
    extent_rows = partition_boxes[:, 0]
    extent_cols = partition_boxes[:, 1]
    table_rows = cosine_table(extent_rows, B)
    table_cols = cosine_table(extent_cols, B)
    table_depth = cosine_table(jnp.full((), total_planes, jnp.int32), total_planes)
    layers = to_cells(table_rows, table_cols, modes_now, B)
    pressure = depth_mix(layers, table_depth.T)
    forcing = interfaces(layers, face_table, extent_rows, extent_cols)
    force_modes = to_modes(table_rows, table_cols, forcing, B)
    first_plane = lax.axis_index("height") * planes
    new_modes = advance(
        modes_now, modes_prev, force_modes, extent_rows, extent_cols, first_plane, total_planes, B
    )
    return (new_modes, pressure)


def solution(mesh):
    placed = (P("height", "dom", None), P("height", "dom", None), P("dom", None), P("dom", None))
    return jax.shard_map(
        on_device,
        mesh=mesh,
        in_specs=placed,
        out_specs=(P("height", "dom", None), P("height", "dom", None)),
        check_vma=False,
    )
```

```python
import jax
import jax.numpy as jnp
from jax import lax
from jax.experimental import pallas as pl
from jax.experimental.pallas import tpu as pltpu
from jax.sharding import PartitionSpec as P

B = 64


COUPLING = 32.0
STENCIL = (COUPLING * 270.0 / 180.0, COUPLING * -27.0 / 180.0, COUPLING * 2.0 / 180.0)
TIME_STEP = 0.4
SERIES = (1.0, -1.0 / 6, 1.0 / 120, -1.0 / 5040, 1.0 / 362880, -1.0 / 39916800, 1.0 / 6227020800)


def cosine_table(lengths, box_side):
    lengths = lengths.astype(jnp.float32)[..., None, None]
    ordinal = jnp.arange(box_side, dtype=jnp.float32)
    waves = ordinal[:, None]
    places = ordinal[None, :]
    scales = jnp.sqrt(jnp.where(waves == 0, 1.0, 2.0) / lengths)
    values = scales * jnp.cos(jnp.pi * waves * (places + 0.5) / lengths)
    inside = (waves < lengths) & (places < lengths)
    return jnp.where(inside, values, 0.0)


def to_modes(table_rows, table_cols, grid_field, box_side):
    planes, holders, cells = grid_field.shape
    squares = grid_field.reshape(planes, holders, box_side, box_side)
    halfway = jnp.einsum("pka,zpab->zpkb", table_rows, squares, precision=lax.Precision.HIGH)
    complete = jnp.einsum("zpkb,plb->zpkl", halfway, table_cols, precision=lax.Precision.HIGH)
    return complete.reshape(planes, holders, cells)


def mix_kernel(m_ref, x_ref, o_ref):
    for p in range(x_ref.shape[1]):
        x = x_ref[:, p, :]
        xh = x.astype(jnp.bfloat16)
        xl = (x - xh.astype(jnp.float32)).astype(jnp.bfloat16)
        o_ref[:, p, :] = jnp.dot(
            m_ref[...], jnp.concatenate([xh, xl, xh], 0), preferred_element_type=jnp.float32
        )


def depth_mix(grid_field, matrix):
    shares, planes, holders, width = grid_field.shape
    total = shares * planes
    pieces = lax.all_to_all(grid_field, "height", split_axis=0, concat_axis=0, tiled=True)
    mh, ml = split(matrix)
    step = min(width, 512)
    combined = pl.pallas_call(
        mix_kernel,
        grid=(width // step,),
        in_specs=[
            pl.BlockSpec((total, 3 * total), lambda i: (0, 0)),
            pl.BlockSpec((total, holders, step), lambda i: (0, 0, i)),
        ],
        out_specs=pl.BlockSpec((total, holders, step), lambda i: (0, 0, i)),
        out_shape=jax.ShapeDtypeStruct((total, holders, width), jnp.float32),
        name="depth",
        cost_estimate=pl.CostEstimate(
            flops=2 * total * total * holders * width,
            bytes_accessed=8 * total * holders * width,
            transcendentals=0,
        ),
    )(jnp.concatenate([mh, mh, ml], 1), pieces.reshape(total, holders, width))
    received = lax.all_to_all(
        combined.reshape(grid_field.shape), "height", split_axis=0, concat_axis=0, tiled=True
    )
    return received.transpose(1, 2, 0, 3).reshape(planes, holders, shares * width)


def split(values):
    high = lax.reduce_precision(values, 8, 7)
    return high.astype(jnp.bfloat16), (values - high).astype(jnp.bfloat16)


GROUP = 4


def cells_kernel(x_ref, w_ref, c_ref, q_ref, sr_ref, sc_ref):
    group, holders, cells = x_ref.shape
    half = B // 2
    low = lax.broadcasted_iota(jnp.int32, (half, 2 * B), 1) < B
    planes = [x_ref[z].reshape(holders, half, 2 * B) for z in range(group)]
    outs = [[] for _ in range(group)]
    for p in range(holders):
        cols = []
        for k in range(group // 2):
            one, two = planes[2 * k][p], planes[2 * k + 1][p]
            top = jnp.where(low, one, pltpu.roll(two, B, 1))
            bottom = jnp.where(low, pltpu.roll(one, B, 1), two)
            cols.append(jnp.concatenate([top, bottom], 0))
        u = jnp.concatenate(cols, 1)
        uh = u.astype(jnp.bfloat16)
        ul = (u - uh.astype(jnp.float32)).astype(jnp.bfloat16)
        v = jnp.dot(
            w_ref[p], jnp.concatenate([uh, ul, uh], 0), preferred_element_type=jnp.float32
        )
        v = jnp.concatenate([v[:, 2 * B * k : 2 * B * (k + 1)] for k in range(group // 2)], 0)
        vh = v.astype(jnp.bfloat16)
        vl = (v - vh.astype(jnp.float32)).astype(jnp.bfloat16)
        q = jnp.dot(
            jnp.concatenate([vh, vl, vh], 1), c_ref[p], preferred_element_type=jnp.float32
        )
        rows = B + 16
        for k in range(group // 2):
            top = q[rows * k : rows * k + half, : 2 * B]
            bottom = q[rows * k + half : rows * k + B, : 2 * B]
            outs[2 * k].append(jnp.where(low, top, pltpu.roll(bottom, B, 1)))
            outs[2 * k + 1].append(jnp.where(low, pltpu.roll(top, B, 1), bottom))
            sr_ref[k, p] = q[rows * k + B : rows * k + B + 8, : 2 * B]
            sc_ref[k, p] = jnp.transpose(q[rows * k : rows * k + B, 2 * B :])[:16]
    for z in range(group):
        plane = jnp.stack(outs[z], 0).reshape(holders, cells)
        width = q_ref.shape[-1]
        for h in range(q_ref.shape[0]):
            q_ref[h, z] = plane[:, h * width : (h + 1) * width]


def cells_and_sides(modes, table_rows, table_cols, select_rows, select_cols):
    planes, holders, cells = modes.shape
    order = jnp.concatenate([jnp.arange(0, B, 2), jnp.arange(1, B, 2)])
    exact = lax.Precision.HIGHEST
    pick_r = jnp.pad(select_rows.reshape(holders, 6, B), ((0, 0), (0, 10), (0, 0)))
    pick_c = jnp.pad(select_cols.reshape(holders, 6, B), ((0, 0), (0, 2), (0, 0)))
    side_r = jnp.einsum("psx,pkx->psk", pick_r, table_rows, precision=exact)
    side_c = jnp.einsum("psy,pky->pks", pick_c, table_cols, precision=exact)
    weights = jnp.concatenate([table_rows.swapaxes(1, 2)[:, order], side_r], 1)[:, :, order]
    wh, wl = split(weights)
    weights = jnp.concatenate([wh, wh, wl], 2)
    blank = jnp.zeros_like(table_cols)
    none = jnp.zeros_like(side_c)
    tail = jnp.zeros((holders, B, 2 * B - 16), jnp.float32)
    upper = jnp.concatenate([table_cols, blank, side_c, none, tail], 2)
    lower = jnp.concatenate([blank, table_cols, none, side_c, tail], 2)
    ch, cl = split(jnp.concatenate([upper, lower], 1))
    columns = jnp.concatenate([ch, ch, cl], 1)
    pairs = planes // 2
    shares = lax.axis_size("height")
    whole = lambda shape: pl.BlockSpec(shape, lambda i: (0,) * len(shape))
    q, sr, sc = pl.pallas_call(
        cells_kernel,
        grid=(planes // GROUP,),
        in_specs=[
            pl.BlockSpec((GROUP, holders, cells), lambda i: (i, 0, 0)),
            whole(weights.shape),
            whole(columns.shape),
        ],
        out_specs=[
            pl.BlockSpec((shares, GROUP, holders, cells // shares), lambda i: (0, i, 0, 0)),
            pl.BlockSpec((GROUP // 2, holders, 8, 2 * B), lambda i: (i, 0, 0, 0)),
            pl.BlockSpec((GROUP // 2, holders, 16, B), lambda i: (i, 0, 0, 0)),
        ],
        out_shape=[
            jax.ShapeDtypeStruct((shares, planes, holders, cells // shares), jnp.float32),
            jax.ShapeDtypeStruct((pairs, holders, 8, 2 * B), jnp.float32),
            jax.ShapeDtypeStruct((pairs, holders, 16, B), jnp.float32),
        ],
        name="cells",
        cost_estimate=pl.CostEstimate(
            flops=4 * planes * holders * B**3, bytes_accessed=8 * planes * holders * cells, transcendentals=0
        ),
    )(modes, weights, columns)
    sr = sr.reshape(pairs, holders, 8, 2, B)[:, :, :6].transpose(0, 3, 1, 2, 4)
    sc = sc.reshape(pairs, holders, 2, 8, 2, B // 2)[:, :, :, :6].transpose(0, 2, 1, 3, 5, 4)
    sides = jnp.concatenate(
        [sr.reshape(planes, holders, 2, 3 * B), sc.reshape(planes, holders, 2, 3 * B)], 2
    )
    return q, sides.reshape(planes, holders * 4, 3 * B)


def side_selectors(extent_rows, extent_cols, box_side):
    holders = extent_rows.shape[0]
    layers = jnp.arange(3, dtype=jnp.int32)[None, :, None]
    place = jnp.arange(box_side, dtype=jnp.int32)[None, None, :]
    lowest = jnp.broadcast_to(place == layers, (holders, 3, box_side))
    high_rows = place == extent_rows[:, None, None] - 1 - layers
    high_cols = place == extent_cols[:, None, None] - 1 - layers
    select_rows = jnp.stack([lowest, high_rows], 1).astype(jnp.float32)
    select_cols = jnp.stack([lowest, high_cols], 1).astype(jnp.float32)
    return (select_rows, select_cols)


def shifter(offsets, amounts, box_side):
    spot = jnp.arange(box_side, dtype=jnp.int32)[None, :, None]
    cellpos = jnp.arange(box_side, dtype=jnp.int32)[None, None, :]
    hits = (cellpos == offsets[:, None, None] + spot) & (spot < amounts[:, None, None])
    return hits.astype(jnp.float32)


def pick_rows(row_ids, count):
    return (row_ids[:, None] == jnp.arange(count, dtype=jnp.int32)[None, :]).astype(jnp.float32)


def select_faces(stacked, row_ids, offsets, amounts, box_side):
    planes, count, width = stacked.shape
    picked = jnp.einsum(
        "rk,zkm->zrm", pick_rows(row_ids, count), stacked, precision=lax.Precision.HIGH
    )
    picked = picked.reshape(planes, row_ids.shape[0], 3, box_side)
    return jnp.einsum(
        "rqc,zrjc->zrjq",
        shifter(offsets, amounts, box_side),
        picked,
        precision=lax.Precision.HIGH,
    )


def face_forcing(
    local_sides, aligned, targets, facing, offsets, amounts, select_rows, select_cols, box_side
):
    planes, count, width = local_sides.shape
    holders = count // 4
    number = targets.shape[0]
    target_ids = targets * 4 + facing
    inside_rim = select_faces(local_sides, target_ids, offsets, amounts, box_side)
    jumps = aligned - inside_rim
    nearest = jumps[:, :, 0]
    second = jumps[:, :, 1]
    farthest = jumps[:, :, 2]
    closest = STENCIL[0] * nearest + STENCIL[1] * second + STENCIL[2] * farthest
    middle = STENCIL[1] * nearest + STENCIL[2] * second
    outer = STENCIL[2] * nearest
    pushes = jnp.stack([closest, middle, outer], 2)
    placed = jnp.einsum(
        "rqc,zrjq->zrjc",
        shifter(offsets, amounts, box_side),
        pushes,
        precision=lax.Precision.HIGH,
    )
    placed = placed.reshape(planes, number, 3 * box_side)
    side_force = jnp.einsum(
        "rk,zrm->zkm", pick_rows(target_ids, count), placed, precision=lax.Precision.HIGH
    )
    side_force = side_force.reshape(planes, holders, 4, 3, box_side)
    from_cols = jnp.einsum(
        "psjx,zpsjy->zpxy", select_rows, side_force[:, :, 0:2], precision=lax.Precision.HIGH
    )
    from_rows = jnp.einsum(
        "psjy,zpsjx->zpxy", select_cols, side_force[:, :, 2:4], precision=lax.Precision.HIGH
    )
    return (from_cols + from_rows).reshape(planes, holders, box_side * box_side)


def interfaces(local_sides, face_table, select_rows, select_cols):
    planes = local_sides.shape[0]
    listed = face_table.shape[0]
    dom_count = lax.axis_size("dom")
    pair_most = max(2, listed // dom_count)
    source_ids = face_table[:, 0] * 4 + face_table[:, 1]
    rim_values = select_faces(
        local_sides, source_ids, face_table[:, 2], face_table[:, 3], B
    ).reshape(planes, listed, 3 * B)
    targets = face_table[:, 4]
    matches = (targets[:, None] == jnp.arange(dom_count, dtype=jnp.int32)[None, :]).astype(
        jnp.int32
    )
    position_in = jnp.sum(jnp.cumsum(matches, 0) * matches, 1) - 1
    slot_ids = targets * pair_most + position_in
    slot_hits = (
        jnp.arange(dom_count * pair_most, dtype=jnp.int32)[:, None] == slot_ids[None, :]
    ).astype(jnp.int32)
    outgoing = jnp.einsum(
        "sr,zrm->zsm", slot_hits.astype(jnp.float32), rim_values, precision=lax.Precision.HIGH
    )
    labels = jnp.stack([face_table[:, 5], face_table[:, 6], face_table[:, 7], face_table[:, 3]], 1)
    label_slots = jnp.sum(slot_hits[:, :, None] * labels[None, :, :], 1)[None]
    label_plane = jnp.pad(label_slots.astype(jnp.float32), ((0, 0), (0, 0), (0, 3 * B - 4)))
    received = lax.all_to_all(
        jnp.concatenate([outgoing, label_plane], 0), "dom", split_axis=1, concat_axis=1, tiled=True
    )
    arrived = received[planes, :, :4].astype(jnp.int32)
    aligned = received[:planes].reshape(planes, dom_count * pair_most, 3, B)
    targets_here = arrived[:, 0]
    facing = arrived[:, 1]
    offsets = arrived[:, 2]
    lengths = arrived[:, 3]
    return face_forcing(
        local_sides, aligned, targets_here, facing, offsets, lengths, select_rows, select_cols, B
    )


def advance(
    modes_now,
    modes_prev,
    force_modes,
    extent_rows,
    extent_cols,
    first_plane,
    total_planes,
    box_side,
):
    planes, holders, cells = modes_now.shape
    wave_depth = (first_plane + jnp.arange(planes, dtype=jnp.int32)).astype(
        jnp.float32
    ) / total_planes
    wave_side = jnp.arange(box_side, dtype=jnp.float32)
    float_rows = extent_rows.astype(jnp.float32)
    float_cols = extent_cols.astype(jnp.float32)
    ratio_rows = wave_side[None, :] / float_rows[:, None]
    ratio_cols = wave_side[None, :] / float_cols[:, None]
    quarter = (jnp.pi * TIME_STEP / 2) ** 2 * (
        wave_depth[:, None, None, None] ** 2
        + ratio_rows[None, :, :, None] ** 2
        + ratio_cols[None, :, None, :] ** 2
    )
    ratio = jnp.float32(SERIES[-1])
    for coefficient in SERIES[-2::-1]:
        ratio = ratio * quarter + coefficient
    ratio = ratio * ratio
    growth = TIME_STEP * TIME_STEP * ratio
    inside = (wave_side[None, :, None] < float_rows[:, None, None]) & (
        wave_side[None, None, :] < float_cols[:, None, None]
    )
    grid_shape = (planes, holders, box_side, box_side)
    updated = (
        (2.0 - 4.0 * quarter * ratio) * modes_now.reshape(grid_shape)
        - modes_prev.reshape(grid_shape)
        + growth * force_modes.reshape(grid_shape)
    )
    return jnp.where(inside[None], updated, 0.0).reshape(planes, holders, cells)


def on_device(modes_now, modes_prev, partition_boxes, face_table):
    planes = modes_now.shape[0]
    total_planes = planes * lax.axis_size("height")
    extent_rows = partition_boxes[:, 0]
    extent_cols = partition_boxes[:, 1]
    table_rows = cosine_table(extent_rows, B)
    table_cols = cosine_table(extent_cols, B)
    table_depth = cosine_table(jnp.full((), total_planes, jnp.int32), total_planes)
    select_rows, select_cols = side_selectors(extent_rows, extent_cols, B)
    layers, local_sides = cells_and_sides(
        modes_now, table_rows, table_cols, select_rows, select_cols
    )
    pressure = depth_mix(layers, table_depth.T)
    forcing = interfaces(local_sides, face_table, select_rows, select_cols)
    force_modes = to_modes(table_rows, table_cols, forcing, B)
    first_plane = lax.axis_index("height") * planes
    new_modes = advance(
        modes_now, modes_prev, force_modes, extent_rows, extent_cols, first_plane, total_planes, B
    )
    return (new_modes, pressure)


def solution(mesh):
    placed = (P("height", "dom", None), P("height", "dom", None), P("dom", None), P("dom", None))
    return jax.shard_map(
        on_device,
        mesh=mesh,
        in_specs=placed,
        out_specs=(P("height", "dom", None), P("height", "dom", None)),
        check_vma=False,
    )
```
